32 devices in a mesh: gx: 4 (over x, core), gy: 4 (over z), gz: 2 (over y).
Axes of the slice: x: 2, y: 2, z: 4, core: 2. Of those that a mesh axis runs over, the one named last changes fastest.
Arguments:
- features: float32 [64, 64, 64, 128], P('gx', 'gy', 'gz'), may hold values from -6 to 6
- scales: float32 [64, 64, 64], P('gx', 'gy', 'gz'), may hold values from 0.2 to 0.4
- thetas: float32 [2, 4, 128], replicated, may hold values from -1 to 1
- weights: float32 [2, 128, 128], replicated, may hold values from -0.5 to 0.5
Outputs:
- hidden: float32 [64, 64, 64, 128], P('gx', 'gy', 'gz')
The draws below stay inside these ranges and needn't reach their ends.
All inputs are finite; a program needn't handle non-finite values.
Results may differ from the reference program's by a relative error of at most 0.00011.
Values sent between devices are 32-bit elements; how exact they have to be, the bound alone decides.
A program may use at most 64 MiB of HBM per device.

```python
import jax
import jax.numpy as jnp
from jax import lax

C = 128
ORDER = 3
LAYERS = 2
NX = 64
NY = 64
NZ = 64


def levels(key, extent, split, low, top_value):
    def one(dim, shards_of):
        draws = jax.random.uniform(jax.random.fold_in(jax.random.fold_in(key, 6), dim), (shards_of,), jnp.float32, low / len(split), top_value / len(split))
        return jnp.repeat(jnp.exp(draws), extent[dim] // shards_of).reshape((-1,) + (1,) * (len(extent) - dim - 1))

    gain = one(*split[0])
    for cut in split[1:]:
        gain = gain * one(*cut)
    return gain


def gaussian(rng, shape, deviation, most, pieces=(), kind=jnp.bfloat16):
    level = levels(rng, shape, pieces, -0.22, 0.18) if pieces else 1.0
    drawn = jax.random.normal(rng, shape, jnp.float32) * deviation * level
    return jnp.minimum(jnp.maximum(drawn, -most), most).astype(kind)


def setup_inputs(seed: int = 0) -> dict:
    key_of = jax.random.split(jax.random.key(seed), 5)
    return {
        "features": gaussian(key_of[0], (NX, NY, NZ, C), 1.0, 6.0, ((0, 4), (1, 4), (2, 2)), jnp.float32),
        "scales": jnp.clip(0.2 + 0.2 * jax.random.uniform(key_of[1], (NX, NY, NZ), jnp.float32) ** levels(key_of[1], (NX, NY, NZ), ((0, 4), (1, 4), (2, 2)), -0.2, 0.2), 0.2, 0.4),
        "thetas": jnp.clip(jax.random.uniform(key_of[2], (LAYERS, ORDER + 1, C), jnp.float32, -1.0, 1.0), -1.0, 1.0),
        "weights": gaussian(key_of[3], (LAYERS, C, C), C ** -0.5, 0.5, (), jnp.float32),
    }


def neighbour_sum(scaled):
    total = jnp.roll(scaled, 1, 0) + jnp.roll(scaled, -1, 0)
    total = total + jnp.roll(scaled, 1, 1) + jnp.roll(scaled, -1, 1)
    total = total + jnp.roll(scaled, 1, 2) + jnp.roll(scaled, -1, 2)
    return total


def operate(values_in, scales):
    scaled = scales[..., None] * values_in
    return -scales[..., None] * neighbour_sum(scaled)


def reference(features, scales, thetas, weights):
    hidden = features
    for layer_index in range(LAYERS):
        prior_term = hidden
        this_term = operate(hidden, scales)
        total = thetas[layer_index, 0] * prior_term + thetas[layer_index, 1] * this_term
        for order_index in range(2, ORDER + 1):
            next_term = 2.0 * operate(this_term, scales) - prior_term
            total = total + thetas[layer_index, order_index] * next_term
            prior_term, this_term = this_term, next_term
        flat = total.reshape(-1, total.shape[-1])
        mixed = jnp.dot(flat, weights[layer_index], precision=lax.Precision.HIGHEST, preferred_element_type=jnp.float32)
        hidden = jax.nn.silu(mixed).reshape(total.shape)
    return hidden
```

```python
import functools

import jax
import jax.numpy as jnp
import numpy as np
from jax import lax
from jax.experimental import pallas as pl
from jax.experimental.pallas import tpu as pltpu
from jax.sharding import PartitionSpec as P

MESH = pl.DeviceIdType.MESH
AXES = ("gx", "gy", "gz")
PLANE_GROUPS = 4
HELD = 2


def power_coefficients(order):
    table = np.zeros((order + 1, order + 1))
    table[0, 0] = 1.0
    if order > 0:
        table[1, 1] = 1.0
    for k in range(2, order + 1):
        table[k, 1:] = 2.0 * table[k - 1, :-1]
        table[k] -= table[k - 2]
    return table


def split_weights(w):
    high = w.astype(jnp.bfloat16)
    low = (w - high.astype(jnp.float32)).astype(jnp.bfloat16)
    top = jnp.concatenate([high, low], axis=1)
    bottom = jnp.concatenate([high, jnp.zeros_like(low)], axis=1)
    return jnp.concatenate([top, bottom], axis=0)


def silu(v):
    return v / (1.0 + jnp.exp(-v))


def product(total, packed):
    c = total.shape[-1]
    high = total.astype(jnp.bfloat16)
    low = (total - high.astype(jnp.float32)).astype(jnp.bfloat16)
    out = jnp.dot(
        jnp.concatenate([high, low], axis=1), packed, preferred_element_type=jnp.float32
    )
    return out[:, :c] + out[:, c:]


def diffuse_kernel(
    sizes, features, scales_in, thetas_in, weights_in, out,
    scales, thetas, weights, h, sb, q, zs, zh, wp, tt, in_sem, send_sem, recv_sem, ready,
):
    (nx, ny, nz, c), layers, order = sizes
    table = power_coefficients(order)
    position = {a: lax.axis_index(a) for a in AXES}

    def near(axis, step):
        size = lax.axis_size(axis)
        return {axis: lax.rem(position[axis] + step + size, size)}

    def leads(axis, side):
        last = lax.axis_size(axis) - 1
        return jnp.where(side == 1, position[axis] == last, position[axis] > 0)

    inner = nx - 2
    cuts = [1 + (inner * g) // PLANE_GROUPS for g in range(PLANE_GROUPS + 1)]
    groups = [(cuts[g], cuts[g + 1]) for g in range(PLANE_GROUPS)]
    faces, middle = (0, ny - 1), tuple(range(1, ny - 1))

    pieces = [(slice(0, nx), y, y + 1) for y in faces]
    pieces += [(slice(a, b), 1, ny - 1) for a, b in [(0, 1), (nx - 1, nx)] + groups]
    loads = []
    for i, (xs, a, b) in enumerate(pieces):
        part = (pl.ds(xs.start, xs.stop - xs.start), pl.ds(a, b - a))
        loads.append(pltpu.make_async_copy(features.at[part], h.at[part], in_sem.at[i]))
    small = [
        pltpu.make_async_copy(src, dst, in_sem.at[len(loads) + i])
        for i, (src, dst) in enumerate(
            [(scales_in, scales), (thetas_in, thetas), (weights_in, weights)]
        )
    ]
    barrier = pltpu.get_barrier_semaphore()
    for axis in AXES:
        for side in (0, 1):
            @pl.when(jnp.logical_not(leads(axis, side)))
            def _():
                pl.semaphore_signal(
                    barrier, inc=1, device_id=near(axis, 2 * side - 1), device_id_type=MESH
                )
    for load in small[:2] + loads + small[2:]:
        load.start()
    leaders = sum(leads(axis, side).astype(jnp.int32) for axis in AXES for side in (0, 1))

    @pl.when(leaders > 0)
    def _():
        pl.semaphore_wait(barrier, leaders)

    for a, axis in enumerate(AXES):
        for side in (0, 1):
            @pl.when(leads(axis, side))
            def _():
                pl.semaphore_signal(
                    ready.at[a, 1 - side], inc=1, device_id=near(axis, 2 * side - 1),
                    device_id_type=MESH,
                )

    def meet(a, side):
        @pl.when(jnp.logical_not(leads(AXES[a], side)))
        def _():
            pl.semaphore_wait(ready.at[a, side], 1)

    gy_last = lax.axis_size("gy") - 1
    outer = jnp.logical_or(position["gy"] == 0, position["gy"] == gy_last)
    first = outer.astype(jnp.int32)

    def messages(round_index):
        p = round_index % 2
        made = {}

        def add(key, src, dst, axis, side, m=None):
            m = len(made) if m is None else m
            made[key] = pltpu.make_async_remote_copy(
                src_ref=src, dst_ref=dst, send_sem=send_sem.at[p, m], recv_sem=recv_sem.at[p, m],
                device_id=near(axis, 2 * side - 1), device_id_type=MESH,
            )

        def along(key, xs):
            m = len(made)
            for turn in (0, 1):
                side = first if turn == 0 else 1 - first
                src, dst = 1 + side * (ny - 1), (1 - side) * (ny + 1)
                add(key + (turn,), q.at[p, xs, src], q.at[p, xs, dst], "gy", side, m + side)

        ys = pl.ds(1, ny)
        pair = pl.ds(0, 2)
        for e, x in enumerate((1, nx)):
            along(("ye", e), x)
        add(("x", 0), q.at[p, 1, ys], q.at[p, nx + 1, ys], "gx", 0)
        add(("x", 1), q.at[p, nx, ys], q.at[p, 0, ys], "gx", 1)
        for side in (0, 1):
            add(("ze", side), zs.at[p, side, pair], zh.at[p, 1 - side, pair], "gz", side)
        for g, (a, b) in enumerate(groups):
            xs = pl.ds(1 + a, b - a)
            along(("y", g), xs)
            for side in (0, 1):
                add(("z", side, g), zs.at[p, side, xs], zh.at[p, 1 - side, xs], "gz", side)
        return made

    def coefficient(layer, k):
        total = None
        for t in range(order + 1):
            if table[t, k] != 0.0:
                term = float(table[t, k]) * thetas[layer, pl.ds(t, 1), :]
                total = term if total is None else total + term
        return total

    sublane = lax.broadcasted_iota(jnp.int32, (nz, c), 0)

    def neighbours(p, x, xo, y):
        v = q[p, x + 1, y + 1]
        below = jnp.where(sublane == 0, zh[p, 0, xo, pl.ds(y, 1), :], pltpu.roll(v, 1, 0))
        above = jnp.where(sublane == nz - 1, zh[p, 1, xo, pl.ds(y, 1), :], pltpu.roll(v, nz - 1, 0))
        return (
            (q[p, x, y + 1] + q[p, x + 2, y + 1])
            + (q[p, x + 1, y] + q[p, x + 1, y + 2])
            + (below + above)
        )

    def put(p, x, xo, y, value):
        q[p, x + 1, y + 1] = value
        zs[p, 0, xo, pl.ds(y, 1), :] = value[0:1]
        zs[p, 1, xo, pl.ds(y, 1), :] = value[nz - 1 : nz]

    stages = layers * order + 1

    def compute(stage, x, xo, ys):
        layer, k = divmod(stage, order)
        p_in, p_out = (stage - 1) % 2, stage % 2
        if stage == 0:
            lead = coefficient(0, order)
            for a, b in ((y, y + 1) for y in ys) if len(ys) == 2 else ((ys[0], ys[-1] + 1),):
                sb[x, a:b] = jnp.broadcast_to(scales[x, a:b][:, :, None], (b - a, nz, c))
            for y in ys:
                put(p_out, x, xo, y, sb[x, y] * (lead * h[x, y]))
        elif k != 0:
            ck = coefficient(layer, order - k)
            for y in ys:
                s = sb[x, y]
                put(p_out, x, xo, y, s * (ck * h[x, y] - s * neighbours(p_in, x, xo, y)))
        else:
            c0 = coefficient(layer - 1, 0)
            for i, y in enumerate(ys):
                tt[pl.ds(i * nz, nz)] = c0 * h[x, y] - sb[x, y] * neighbours(p_in, x, xo, y)
            mixed = product(tt[0 : len(ys) * nz], wp[layer - 1])
            mixed = silu(mixed)
            if stage == stages - 1:
                for i, y in enumerate(ys):
                    out[x, y] = mixed[i * nz : (i + 1) * nz]
            else:
                lead = coefficient(layer, order)
                for i, y in enumerate(ys):
                    value = mixed[i * nz : (i + 1) * nz]
                    h[x, y] = value
                    put(p_out, x, xo, y, sb[x, y] * (lead * value))

    def edge_part(stage, ys):
        @pl.loop(0, 2)
        def _(e):
            compute(stage, e * (nx - 1), e, ys)

    def group_part(stage, g, ys):
        @pl.loop(*groups[g])
        def _(x):
            compute(stage, x, x + 1, ys)

    plan = [
        (
            edge_part,
            [("ye", e, turn) for turn in (0, 1) for e in (0, 1)],
            [("x", 0), ("x", 1), ("ze", 0), ("ze", 1)],
        )
    ]
    for g in range(PLANE_GROUPS):
        plan.append(
            (
                functools.partial(lambda g, stage, ys: group_part(stage, g, ys), g),
                [("y", g, turn) for turn in (0, 1)],
                [("z", side, g) for side in (0, 1)],
            )
        )

    history = {}
    held = []
    for stage in range(stages):
        if stage >= 2:
            for copy in history[stage - 2].values():
                copy.wait_send()
        if stage == stages - 1:
            for part, _, others in plan:
                for key in others:
                    history[stage - 1][key].wait_recv()
                part(stage, middle)
            for part, along, _ in plan:
                for key in along:
                    history[stage - 1][key].wait_recv()
                part(stage, faces)
            continue
        now = history[stage] = messages(stage)
        if stage == 1:
            small[2].wait()
            for layer in range(layers):
                wp[layer] = split_weights(weights[layer])
        if stage == 0:
            small[0].wait()
            small[1].wait()
            loads[0].wait()
            loads[1].wait()
            for i, (part, along, _) in enumerate(plan):
                part(stage, faces)
                if i == 0:
                    meet(1, first)
                for key in along:
                    if key[-1] == 0:
                        now[key].start()
            meet(1, 1 - first)
            for _, along, _ in plan:
                for key in along:
                    if key[-1] == 1:
                        now[key].start()
        for i, (part, along, others) in enumerate(plan):
            if stage == 0:
                for load in loads[2:4] if i == 0 else loads[3 + i : 4 + i]:
                    load.wait()
            else:
                for key in others + along:
                    history[stage - 1][key].wait_recv()
                part(stage, faces)
                for key in along:
                    if key[-1] == 0:
                        now[key].start()
                held += [now[key] for key in along if key[-1] == 1]
                while len(held) > (0 if i == len(plan) - 1 else HELD):
                    held.pop(0).start()
            part(stage, middle)
            if stage == 0 and i == 0:
                for a in (0, 2):
                    for side in (0, 1):
                        meet(a, side)
            for key in others:
                now[key].start()
    for copy in history[stages - 2].values():
        copy.wait_send()


def per_device(features, scales, thetas, weights):
    nx, ny, nz, c = features.shape
    layers, order = weights.shape[0], thetas.shape[1] - 1
    count = 8 + 4 * PLANE_GROUPS
    f32 = jnp.float32
    hbm = pl.BlockSpec(memory_space=pl.ANY)
    return pl.pallas_call(
        functools.partial(diffuse_kernel, ((nx, ny, nz, c), layers, order)),
        out_shape=pltpu.VMEM(features.shape, f32),
        in_specs=[hbm] * 4,
        out_specs=pl.BlockSpec(memory_space=pltpu.VMEM),
        scratch_shapes=[
            pltpu.VMEM(scales.shape, f32),
            pltpu.VMEM(thetas.shape, f32),
            pltpu.VMEM(weights.shape, f32),
            pltpu.VMEM((nx, ny, nz, c), f32),
            pltpu.VMEM((nx, ny, nz, c), f32),
            pltpu.VMEM((2, nx + 2, ny + 2, nz, c), f32),
            pltpu.VMEM((2, 2, nx, ny, c), f32),
            pltpu.VMEM((2, 2, nx, ny, c), f32),
            pltpu.VMEM((layers, 2 * c, 2 * c), jnp.bfloat16),
            pltpu.VMEM((ny * nz, c), f32),
            pltpu.SemaphoreType.DMA((PLANE_GROUPS + 7,)),
            pltpu.SemaphoreType.DMA((2, count)),
            pltpu.SemaphoreType.DMA((2, count)),
            pltpu.SemaphoreType.REGULAR((3, 2)),
        ],
        compiler_params=pltpu.CompilerParams(
            collective_id=0, has_side_effects=True, vmem_limit_bytes=62_783_488
        ),
        name="diffuse",
    )(features, scales, thetas, weights)


def solution(mesh):
    return jax.shard_map(
        per_device,
        mesh=mesh,
        in_specs=(P("gx", "gy", "gz", None), P("gx", "gy", "gz"), P(), P()),
        out_specs=P("gx", "gy", "gz", None),
        check_vma=False,
    )
```

```python
import functools

import jax
import jax.numpy as jnp
import numpy as np
from jax import lax
from jax.experimental import pallas as pl
from jax.experimental.pallas import tpu as pltpu
from jax.sharding import PartitionSpec as P

MESH = pl.DeviceIdType.MESH
AXES = ("gx", "gy", "gz")
PLANE_SHARES = (0, 5, 9, 12, 14)
PLANE_GROUPS = len(PLANE_SHARES) - 1
ORDERLY = 2
HOLD = 2


def power_coefficients(order):
    table = np.zeros((order + 1, order + 1))
    table[0, 0] = 1.0
    if order > 0:
        table[1, 1] = 1.0
    for k in range(2, order + 1):
        table[k, 1:] = 2.0 * table[k - 1, :-1]
        table[k] -= table[k - 2]
    return table


def split_weights(w):
    high = w.astype(jnp.bfloat16)
    low = (w - high.astype(jnp.float32)).astype(jnp.bfloat16)
    top = jnp.concatenate([high, low], axis=1)
    bottom = jnp.concatenate([high, jnp.zeros_like(low)], axis=1)
    return jnp.concatenate([top, bottom], axis=0)


def silu(v):
    return v / (1.0 + jnp.exp(-v))


def product(total, packed):
    c = total.shape[-1]
    high = total.astype(jnp.bfloat16)
    low = (total - high.astype(jnp.float32)).astype(jnp.bfloat16)
    out = jnp.dot(
        jnp.concatenate([high, low], axis=1), packed, preferred_element_type=jnp.float32
    )
    return out[:, :c] + out[:, c:]


def diffuse_kernel(
    sizes, features, scales_in, thetas_in, weights_in, out,
    scales, thetas, weights, h, sb, q, zs, zh, wp, tt, in_sem, send_sem, recv_sem, ready,
):
    (nx, ny, nz, c), layers, order = sizes
    table = power_coefficients(order)
    position = {a: lax.axis_index(a) for a in AXES}

    def near(axis, step):
        size = lax.axis_size(axis)
        return {axis: lax.rem(position[axis] + step + size, size)}

    def leads(axis, side):
        last = lax.axis_size(axis) - 1
        return jnp.where(side == 1, position[axis] == last, position[axis] > 0)

    inner = nx - 2
    cuts = [1 + (inner * share) // PLANE_SHARES[-1] for share in PLANE_SHARES]
    groups = [(cuts[g], cuts[g + 1]) for g in range(PLANE_GROUPS)]
    faces, middle = (0, ny - 1), tuple(range(1, ny - 1))

    pieces = [(slice(0, nx), y, y + 1) for y in faces]
    pieces += [(slice(a, b), 1, ny - 1) for a, b in [(0, 1), (nx - 1, nx)] + groups]
    loads = []
    for i, (xs, a, b) in enumerate(pieces):
        part = (pl.ds(xs.start, xs.stop - xs.start), pl.ds(a, b - a))
        loads.append(pltpu.make_async_copy(features.at[part], h.at[part], in_sem.at[i]))
    small = [
        pltpu.make_async_copy(src, dst, in_sem.at[len(loads) + i])
        for i, (src, dst) in enumerate(
            [(scales_in, scales), (thetas_in, thetas), (weights_in, weights)]
        )
    ]
    barrier = pltpu.get_barrier_semaphore()
    for axis in AXES:
        for side in (0, 1):
            @pl.when(jnp.logical_not(leads(axis, side)))
            def _():
                pl.semaphore_signal(
                    barrier, inc=1, device_id=near(axis, 2 * side - 1), device_id_type=MESH
                )
    for load in small[:2] + loads + small[2:]:
        load.start()
    leaders = sum(leads(axis, side).astype(jnp.int32) for axis in AXES for side in (0, 1))

    @pl.when(leaders > 0)
    def _():
        pl.semaphore_wait(barrier, leaders)

    for a, axis in enumerate(AXES):
        for side in (0, 1):
            @pl.when(leads(axis, side))
            def _():
                pl.semaphore_signal(
                    ready.at[a, 1 - side], inc=1, device_id=near(axis, 2 * side - 1),
                    device_id_type=MESH,
                )

    def meet(a, side):
        @pl.when(jnp.logical_not(leads(AXES[a], side)))
        def _():
            pl.semaphore_wait(ready.at[a, side], 1)

    gy_last = lax.axis_size("gy") - 1
    outer = jnp.logical_or(position["gy"] == 0, position["gy"] == gy_last)
    first = outer.astype(jnp.int32)

    def messages(round_index):
        p = round_index % 2
        made = {}

        def add(key, src, dst, axis, side, m=None):
            m = len(made) if m is None else m
            made[key] = pltpu.make_async_remote_copy(
                src_ref=src, dst_ref=dst, send_sem=send_sem.at[p, m], recv_sem=recv_sem.at[p, m],
                device_id=near(axis, 2 * side - 1), device_id_type=MESH,
            )

        def along(key, xs):
            m = len(made)
            for turn in (0, 1):
                side = first if turn == 0 else 1 - first
                src, dst = 1 + side * (ny - 1), (1 - side) * (ny + 1)
                add(key + (turn,), q.at[p, xs, src], q.at[p, xs, dst], "gy", side, m + side)

        ys = pl.ds(1, ny)
        pair = pl.ds(0, 2)
        for e, x in enumerate((1, nx)):
            along(("ye", e), x)
        add(("x", 0), q.at[p, 1, ys], q.at[p, nx + 1, ys], "gx", 0)
        add(("x", 1), q.at[p, nx, ys], q.at[p, 0, ys], "gx", 1)
        for side in (0, 1):
            add(("ze", side), zs.at[p, side, pair], zh.at[p, 1 - side, pair], "gz", side)
        for g, (a, b) in enumerate(groups):
            xs = pl.ds(1 + a, b - a)
            along(("y", g), xs)
            for side in (0, 1):
                add(("z", side, g), zs.at[p, side, xs], zh.at[p, 1 - side, xs], "gz", side)
        return made

    def coefficient(layer, k):
        total = None
        for t in range(order + 1):
            if table[t, k] != 0.0:
                term = float(table[t, k]) * thetas[layer, pl.ds(t, 1), :]
                total = term if total is None else total + term
        return total

    sublane = lax.broadcasted_iota(jnp.int32, (nz, c), 0)

    def neighbours(p, x, xo, y):
        v = q[p, x + 1, y + 1]
        below = jnp.where(sublane == 0, zh[p, 0, xo, pl.ds(y, 1), :], pltpu.roll(v, 1, 0))
        above = jnp.where(sublane == nz - 1, zh[p, 1, xo, pl.ds(y, 1), :], pltpu.roll(v, nz - 1, 0))
        return (
            (q[p, x, y + 1] + q[p, x + 2, y + 1])
            + (q[p, x + 1, y] + q[p, x + 1, y + 2])
            + (below + above)
        )

    def put(p, x, xo, y, value):
        q[p, x + 1, y + 1] = value
        zs[p, 0, xo, pl.ds(y, 1), :] = value[0:1]
        zs[p, 1, xo, pl.ds(y, 1), :] = value[nz - 1 : nz]

    stages = layers * order + 1

    def compute(stage, x, xo, ys):
        layer, k = divmod(stage, order)
        p_in, p_out = (stage - 1) % 2, stage % 2
        if stage == 0:
            lead = coefficient(0, order)
            for a, b in ((y, y + 1) for y in ys) if len(ys) == 2 else ((ys[0], ys[-1] + 1),):
                sb[x, a:b] = jnp.broadcast_to(scales[x, a:b][:, :, None], (b - a, nz, c))
            for y in ys:
                put(p_out, x, xo, y, sb[x, y] * (lead * h[x, y]))
        elif k != 0:
            ck = coefficient(layer, order - k)
            for y in ys:
                s = sb[x, y]
                put(p_out, x, xo, y, s * (ck * h[x, y] - s * neighbours(p_in, x, xo, y)))
        else:
            c0 = coefficient(layer - 1, 0)
            for i, y in enumerate(ys):
                tt[pl.ds(i * nz, nz)] = c0 * h[x, y] - sb[x, y] * neighbours(p_in, x, xo, y)
            mixed = product(tt[0 : len(ys) * nz], wp[layer - 1])
            mixed = silu(mixed)
            if stage == stages - 1:
                for i, y in enumerate(ys):
                    out[x, y] = mixed[i * nz : (i + 1) * nz]
            else:
                lead = coefficient(layer, order)
                for i, y in enumerate(ys):
                    value = mixed[i * nz : (i + 1) * nz]
                    h[x, y] = value
                    put(p_out, x, xo, y, sb[x, y] * (lead * value))

    def edge_part(stage, ys):
        @pl.loop(0, 2)
        def _(e):
            compute(stage, e * (nx - 1), e, ys)

    def group_part(stage, g, ys):
        @pl.loop(*groups[g])
        def _(x):
            compute(stage, x, x + 1, ys)

    plan = [
        (
            edge_part,
            [("ye", e, turn) for turn in (0, 1) for e in (0, 1)],
            [("x", 0), ("x", 1), ("ze", 0), ("ze", 1)],
        )
    ]
    for g in range(PLANE_GROUPS):
        plan.append(
            (
                functools.partial(lambda g, stage, ys: group_part(stage, g, ys), g),
                [("y", g, turn) for turn in (0, 1)],
                [("z", side, g) for side in (0, 1)],
            )
        )

    history = {}
    held, lagged = [], []
    slow = lax.rem(position['gx'], 2) == 1

    def dispatch(copies, wait, queue, limit):
        if wait is None:
            for copy in copies:
                copy.start()
            return

        @pl.when(jnp.logical_not(wait))
        def _():
            for copy in copies:
                copy.start()

        queue += copies
        ready_now = []
        while len(queue) > limit:
            ready_now.append(queue.pop(0))
        if ready_now:
            @pl.when(wait)
            def _():
                for copy in ready_now:
                    copy.start()

    for stage in range(stages):
        if stage >= 2:
            for copy in history[stage - 2].values():
                copy.wait_send()
        if stage == stages - 1:
            for part, _, others in plan:
                for key in others:
                    history[stage - 1][key].wait_recv()
                part(stage, middle)
            for part, along, _ in plan:
                for key in along:
                    history[stage - 1][key].wait_recv()
                part(stage, faces)
            continue
        now = history[stage] = messages(stage)
        if stage == 1:
            small[2].wait()
            for layer in range(layers):
                wp[layer] = split_weights(weights[layer])
        if stage == 0:
            small[0].wait()
            small[1].wait()
            loads[0].wait()
            loads[1].wait()
            for i, (part, along, _) in enumerate(plan):
                part(stage, faces)
                if i == 0:
                    meet(1, first)
                for key in along:
                    if key[-1] == 0:
                        now[key].start()
            meet(1, 1 - first)
            for _, along, _ in plan:
                for key in along:
                    if key[-1] == 1:
                        now[key].start()
        for i, (part, along, others) in enumerate(plan):
            if stage == 0:
                for load in loads[2:4] if i == 0 else loads[3 + i : 4 + i]:
                    load.wait()
            else:
                for key in others + along:
                    history[stage - 1][key].wait_recv()
                part(stage, faces)
                ahead, behind = (
                    [now[key] for key in along if key[-1] == turn] for turn in (0, 1)
                )
                final = i == len(plan) - 1
                dispatch(ahead, slow if stage >= ORDERLY else None, lagged, 0 if final else HOLD)
                dispatch(behind, outer, held, 0 if final else HOLD)
            part(stage, middle)
            if stage == 0 and i == 0:
                for a in (0, 2):
                    for side in (0, 1):
                        meet(a, side)
            for key in others:
                now[key].start()
    for copy in history[stages - 2].values():
        copy.wait_send()


def per_device(features, scales, thetas, weights):
    nx, ny, nz, c = features.shape
    layers, order = weights.shape[0], thetas.shape[1] - 1
    count = 8 + 4 * PLANE_GROUPS
    f32 = jnp.float32
    hbm = pl.BlockSpec(memory_space=pl.ANY)
    return pl.pallas_call(
        functools.partial(diffuse_kernel, ((nx, ny, nz, c), layers, order)),
        out_shape=pltpu.VMEM(features.shape, f32),
        in_specs=[hbm] * 4,
        out_specs=pl.BlockSpec(memory_space=pltpu.VMEM),
        scratch_shapes=[
            pltpu.VMEM(scales.shape, f32),
            pltpu.VMEM(thetas.shape, f32),
            pltpu.VMEM(weights.shape, f32),
            pltpu.VMEM((nx, ny, nz, c), f32),
            pltpu.VMEM((nx, ny, nz, c), f32),
            pltpu.VMEM((2, nx + 2, ny + 2, nz, c), f32),
            pltpu.VMEM((2, 2, nx, ny, c), f32),
            pltpu.VMEM((2, 2, nx, ny, c), f32),
            pltpu.VMEM((layers, 2 * c, 2 * c), jnp.bfloat16),
            pltpu.VMEM((ny * nz, c), f32),
            pltpu.SemaphoreType.DMA((PLANE_GROUPS + 7,)),
            pltpu.SemaphoreType.DMA((2, count)),
            pltpu.SemaphoreType.DMA((2, count)),
            pltpu.SemaphoreType.REGULAR((3, 2)),
        ],
        compiler_params=pltpu.CompilerParams(
            collective_id=0, has_side_effects=True, vmem_limit_bytes=62_783_488
        ),
        name="diffuse",
    )(features, scales, thetas, weights)


def solution(mesh):
    return jax.shard_map(
        per_device,
        mesh=mesh,
        in_specs=(P("gx", "gy", "gz", None), P("gx", "gy", "gz"), P(), P()),
        out_specs=P("gx", "gy", "gz", None),
        check_vma=False,
    )
```

```python
import functools

import jax
import jax.numpy as jnp
import numpy as np
from jax import lax
from jax.experimental import pallas as pl
from jax.experimental.pallas import tpu as pltpu
from jax.sharding import PartitionSpec as P

MESH = pl.DeviceIdType.MESH
AXES = ("gx", "gy", "gz")
PLANE_SHARES = (0, 5, 9, 12, 14)
PLANE_GROUPS = len(PLANE_SHARES) - 1
ORDERLY = 2
HOLD = 2


def power_coefficients(order):
    table = np.zeros((order + 1, order + 1))
    table[0, 0] = 1.0
    if order > 0:
        table[1, 1] = 1.0
    for k in range(2, order + 1):
        table[k, 1:] = 2.0 * table[k - 1, :-1]
        table[k] -= table[k - 2]
    return table


def split_weights(w):
    high = w.astype(jnp.bfloat16)
    low = (w - high.astype(jnp.float32)).astype(jnp.bfloat16)
    top = jnp.concatenate([high, low], axis=1)
    bottom = jnp.concatenate([high, jnp.zeros_like(low)], axis=1)
    return jnp.concatenate([top, bottom], axis=0)


def silu(v):
    return v / (1.0 + jnp.exp(-v))


def product(total, packed):
    c = total.shape[-1]
    high = total.astype(jnp.bfloat16)
    low = (total - high.astype(jnp.float32)).astype(jnp.bfloat16)
    out = jnp.dot(
        jnp.concatenate([high, low], axis=1), packed, preferred_element_type=jnp.float32
    )
    return out[:, :c] + out[:, c:]


def diffuse_kernel(
    sizes, features, scales_in, thetas_in, weights_in, out,
    scales, thetas, weights, h, sb, q, zs, zh, wp, tt, in_sem, send_sem, recv_sem, ready,
):
    (nx, ny, nz, c), layers, order = sizes
    table = power_coefficients(order)
    position = {a: lax.axis_index(a) for a in AXES}

    def near(axis, step):
        size = lax.axis_size(axis)
        return {axis: lax.rem(position[axis] + step + size, size)}

    def leads(axis, side):
        last = lax.axis_size(axis) - 1
        return jnp.where(side == 1, position[axis] == last, position[axis] > 0)

    inner = nx - 2
    cuts = [1 + (inner * share) // PLANE_SHARES[-1] for share in PLANE_SHARES]
    groups = [(cuts[g], cuts[g + 1]) for g in range(PLANE_GROUPS)]
    faces, middle = (0, ny - 1), tuple(range(1, ny - 1))

    pieces = [(slice(0, nx), y, y + 1) for y in faces]
    pieces += [(slice(a, b), 1, ny - 1) for a, b in [(0, 1), (nx - 1, nx)] + groups]
    loads = []
    for i, (xs, a, b) in enumerate(pieces):
        part = (pl.ds(xs.start, xs.stop - xs.start), pl.ds(a, b - a))
        loads.append(pltpu.make_async_copy(features.at[part], h.at[part], in_sem.at[i]))
    small = [
        pltpu.make_async_copy(src, dst, in_sem.at[len(loads) + i])
        for i, (src, dst) in enumerate(
            [(scales_in, scales), (thetas_in, thetas), (weights_in, weights)]
        )
    ]
    barrier = pltpu.get_barrier_semaphore()
    for axis in AXES:
        for side in (0, 1):
            @pl.when(jnp.logical_not(leads(axis, side)))
            def _():
                pl.semaphore_signal(
                    barrier, inc=1, device_id=near(axis, 2 * side - 1), device_id_type=MESH
                )
    for load in small[:2] + loads[:2]:
        load.start()
    leaders = sum(leads(axis, side).astype(jnp.int32) for axis in AXES for side in (0, 1))

    @pl.when(leaders > 0)
    def _():
        pl.semaphore_wait(barrier, leaders)

    for a, axis in enumerate(AXES):
        for side in (0, 1):
            @pl.when(leads(axis, side))
            def _():
                pl.semaphore_signal(
                    ready.at[a, 1 - side], inc=1, device_id=near(axis, 2 * side - 1),
                    device_id_type=MESH,
                )

    for load in loads[2:] + small[2:]:
        load.start()

    def meet(a, side):
        @pl.when(jnp.logical_not(leads(AXES[a], side)))
        def _():
            pl.semaphore_wait(ready.at[a, side], 1)

    gy_last = lax.axis_size("gy") - 1
    outer = jnp.logical_or(position["gy"] == 0, position["gy"] == gy_last)
    first = outer.astype(jnp.int32)

    def messages(round_index):
        p = round_index % 2
        made = {}

        def add(key, src, dst, axis, side, m=None):
            m = len(made) if m is None else m
            made[key] = pltpu.make_async_remote_copy(
                src_ref=src, dst_ref=dst, send_sem=send_sem.at[p, m], recv_sem=recv_sem.at[p, m],
                device_id=near(axis, 2 * side - 1), device_id_type=MESH,
            )

        def along(key, xs):
            m = len(made)
            for turn in (0, 1):
                side = first if turn == 0 else 1 - first
                src, dst = 1 + side * (ny - 1), (1 - side) * (ny + 1)
                add(key + (turn,), q.at[p, xs, src], q.at[p, xs, dst], "gy", side, m + side)

        ys = pl.ds(1, ny)
        pair = pl.ds(0, 2)
        for e, x in enumerate((1, nx)):
            along(("ye", e), x)
        add(("x", 0), q.at[p, 1, ys], q.at[p, nx + 1, ys], "gx", 0)
        add(("x", 1), q.at[p, nx, ys], q.at[p, 0, ys], "gx", 1)
        for side in (0, 1):
            add(("ze", side), zs.at[p, side, pair], zh.at[p, 1 - side, pair], "gz", side)
        for g, (a, b) in enumerate(groups):
            xs = pl.ds(1 + a, b - a)
            along(("y", g), xs)
            for side in (0, 1):
                add(("z", side, g), zs.at[p, side, xs], zh.at[p, 1 - side, xs], "gz", side)
        return made

    def coefficient(layer, k):
        total = None
        for t in range(order + 1):
            if table[t, k] != 0.0:
                term = float(table[t, k]) * thetas[layer, pl.ds(t, 1), :]
                total = term if total is None else total + term
        return total

    sublane = lax.broadcasted_iota(jnp.int32, (nz, c), 0)

    def neighbours(p, x, xo, y):
        v = q[p, x + 1, y + 1]
        below = jnp.where(sublane == 0, zh[p, 0, xo, pl.ds(y, 1), :], pltpu.roll(v, 1, 0))
        above = jnp.where(sublane == nz - 1, zh[p, 1, xo, pl.ds(y, 1), :], pltpu.roll(v, nz - 1, 0))
        return (
            (q[p, x, y + 1] + q[p, x + 2, y + 1])
            + (q[p, x + 1, y] + q[p, x + 1, y + 2])
            + (below + above)
        )

    def put(p, x, xo, y, value):
        q[p, x + 1, y + 1] = value
        zs[p, 0, xo, pl.ds(y, 1), :] = value[0:1]
        zs[p, 1, xo, pl.ds(y, 1), :] = value[nz - 1 : nz]

    stages = layers * order + 1

    def compute(stage, x, xo, ys):
        layer, k = divmod(stage, order)
        p_in, p_out = (stage - 1) % 2, stage % 2
        if stage == 0:
            lead = coefficient(0, order)
            for a, b in ((y, y + 1) for y in ys) if len(ys) == 2 else ((ys[0], ys[-1] + 1),):
                sb[x, a:b] = jnp.broadcast_to(scales[x, a:b][:, :, None], (b - a, nz, c))
            for y in ys:
                put(p_out, x, xo, y, sb[x, y] * (lead * h[x, y]))
        elif k != 0:
            ck = coefficient(layer, order - k)
            for y in ys:
                s = sb[x, y]
                put(p_out, x, xo, y, s * (ck * h[x, y] - s * neighbours(p_in, x, xo, y)))
        else:
            c0 = coefficient(layer - 1, 0)
            for i, y in enumerate(ys):
                tt[pl.ds(i * nz, nz)] = c0 * h[x, y] - sb[x, y] * neighbours(p_in, x, xo, y)
            mixed = product(tt[0 : len(ys) * nz], wp[layer - 1])
            mixed = silu(mixed)
            if stage == stages - 1:
                for i, y in enumerate(ys):
                    out[x, y] = mixed[i * nz : (i + 1) * nz]
            else:
                lead = coefficient(layer, order)
                for i, y in enumerate(ys):
                    value = mixed[i * nz : (i + 1) * nz]
                    h[x, y] = value
                    put(p_out, x, xo, y, sb[x, y] * (lead * value))

    def edge_part(stage, ys):
        @pl.loop(0, 2)
        def _(e):
            compute(stage, e * (nx - 1), e, ys)

    def group_part(stage, g, ys):
        @pl.loop(*groups[g])
        def _(x):
            compute(stage, x, x + 1, ys)

    plan = [
        (
            edge_part,
            [("ye", e, turn) for turn in (0, 1) for e in (0, 1)],
            [("x", 0), ("x", 1), ("ze", 0), ("ze", 1)],
        )
    ]
    for g in range(PLANE_GROUPS):
        plan.append(
            (
                functools.partial(lambda g, stage, ys: group_part(stage, g, ys), g),
                [("y", g, turn) for turn in (0, 1)],
                [("z", side, g) for side in (0, 1)],
            )
        )

    history = {}
    held, lagged = [], []
    slow = lax.rem(position['gx'], 2) == 1

    def dispatch(copies, wait, queue, limit):
        if wait is None:
            for copy in copies:
                copy.start()
            return

        @pl.when(jnp.logical_not(wait))
        def _():
            for copy in copies:
                copy.start()

        queue += copies
        ready_now = []
        while len(queue) > limit:
            ready_now.append(queue.pop(0))
        if ready_now:
            @pl.when(wait)
            def _():
                for copy in ready_now:
                    copy.start()

    for stage in range(stages):
        if stage >= 2:
            for copy in history[stage - 2].values():
                copy.wait_send()
        if stage == stages - 1:
            for part, _, others in plan:
                for key in others:
                    history[stage - 1][key].wait_recv()
                part(stage, middle)
            for part, along, _ in plan:
                for key in along:
                    history[stage - 1][key].wait_recv()
                part(stage, faces)
            continue
        now = history[stage] = messages(stage)
        if stage == 1:
            small[2].wait()
            for layer in range(layers):
                wp[layer] = split_weights(weights[layer])
        if stage == 0:
            small[0].wait()
            small[1].wait()
            loads[0].wait()
            loads[1].wait()
            for i, (part, along, _) in enumerate(plan):
                part(stage, faces)
                if i == 0:
                    meet(1, first)
                for key in along:
                    if key[-1] == 0:
                        now[key].start()
            meet(1, 1 - first)
            for _, along, _ in plan:
                for key in along:
                    if key[-1] == 1:
                        now[key].start()
        for i, (part, along, others) in enumerate(plan):
            if stage == 0:
                for load in loads[2:4] if i == 0 else loads[3 + i : 4 + i]:
                    load.wait()
            else:
                for key in others + along:
                    history[stage - 1][key].wait_recv()
                part(stage, faces)
                ahead, behind = (
                    [now[key] for key in along if key[-1] == turn] for turn in (0, 1)
                )
                final = i == len(plan) - 1
                dispatch(ahead, slow if stage >= ORDERLY else None, lagged, 0 if final else HOLD)
                dispatch(behind, outer, held, 0 if final else HOLD)
            part(stage, middle)
            if stage == 0 and i == 0:
                for a in (0, 2):
                    for side in (0, 1):
                        meet(a, side)
            for key in others:
                now[key].start()
    for copy in history[stages - 2].values():
        copy.wait_send()


def per_device(features, scales, thetas, weights):
    nx, ny, nz, c = features.shape
    layers, order = weights.shape[0], thetas.shape[1] - 1
    count = 8 + 4 * PLANE_GROUPS
    f32 = jnp.float32
    hbm = pl.BlockSpec(memory_space=pl.ANY)
    return pl.pallas_call(
        functools.partial(diffuse_kernel, ((nx, ny, nz, c), layers, order)),
        out_shape=pltpu.VMEM(features.shape, f32),
        in_specs=[hbm] * 4,
        out_specs=pl.BlockSpec(memory_space=pltpu.VMEM),
        scratch_shapes=[
            pltpu.VMEM(scales.shape, f32),
            pltpu.VMEM(thetas.shape, f32),
            pltpu.VMEM(weights.shape, f32),
            pltpu.VMEM((nx, ny, nz, c), f32),
            pltpu.VMEM((nx, ny, nz, c), f32),
            pltpu.VMEM((2, nx + 2, ny + 2, nz, c), f32),
            pltpu.VMEM((2, 2, nx, ny, c), f32),
            pltpu.VMEM((2, 2, nx, ny, c), f32),
            pltpu.VMEM((layers, 2 * c, 2 * c), jnp.bfloat16),
            pltpu.VMEM((ny * nz, c), f32),
            pltpu.SemaphoreType.DMA((PLANE_GROUPS + 7,)),
            pltpu.SemaphoreType.DMA((2, count)),
            pltpu.SemaphoreType.DMA((2, count)),
            pltpu.SemaphoreType.REGULAR((3, 2)),
        ],
        compiler_params=pltpu.CompilerParams(
            collective_id=0, has_side_effects=True, vmem_limit_bytes=62_783_488
        ),
        name="diffuse",
    )(features, scales, thetas, weights)


def solution(mesh):
    return jax.shard_map(
        per_device,
        mesh=mesh,
        in_specs=(P("gx", "gy", "gz", None), P("gx", "gy", "gz"), P(), P()),
        out_specs=P("gx", "gy", "gz", None),
        check_vma=False,
    )
```
